32 devices in a mesh: dp: 1 (over z), tp: 4 (over y), cp: 8 (over x, core).
Axes of the slice: x: 4, y: 4, z: 1, core: 2. Of those that a mesh axis runs over, the one named last changes fastest.
The devices are a block of a 4x4x8 slice.
Arguments:
- x_chunk: bfloat16 [24, 512, 3072], P('dp', 'cp')
- w_query: bfloat16 [3072, 3072], P(None, 'tp')
- w_key: bfloat16 [3072, 1024], P(None, 'tp')
- w_value: bfloat16 [3072, 1024], P(None, 'tp')
- w_out: bfloat16 [3072, 3072], P('tp')
- q_gain: bfloat16 [3072], P('tp')
- k_gain: bfloat16 [1024], P('tp')
- post_gain: bfloat16 [3072], replicated
- cache_k: bfloat16 [24, 8192, 8, 128], P('dp', 'cp', 'tp')
- cache_v: bfloat16 [24, 8192, 8, 128], P('dp', 'cp', 'tp')
- prefix_len: int32 [24], P('dp')
Outputs:
- output 1: bfloat16 [24, 512, 3072], P('dp', 'cp')
- output 2: bfloat16 [24, 512, 8, 128], P('dp', 'cp', 'tp')
- output 3: bfloat16 [24, 512, 8, 128], P('dp', 'cp', 'tp')
All inputs are finite; a program needn't handle non-finite values.
Results may differ from the reference program's by a relative error of at most 0.00713331.
Values are sent between devices in bfloat16 or wider.
A program may use at most 768 MiB of HBM per device.

```python
import jax
import jax.numpy as jnp
from jax import lax

BATCH_ROWS = 24
CHUNK_LEN = 512
CACHE_LEN = 8192
MODEL_DIM = 3072
Q_HEADS = 24
KV_HEADS = 8
HEAD_DIM = 128
QUERY_BLOCK = min(CHUNK_LEN, 16)
ROPE_BASE = 500000.0
NORM_EPS = 1e-6


def head_scales(rng_key, n_heads, trend_slope):
    trend_pos = jnp.arange(n_heads, dtype=jnp.float32) * (2.0 / max(n_heads - 1, 1)) - 1.0
    noise_val = jax.random.normal(rng_key, (n_heads,), jnp.float32)
    return jnp.exp(trend_slope * trend_pos + 0.2 * noise_val)


def draw_prefix(rng_key):
    key_order, key_len = jax.random.split(rng_key)
    row_order = jax.random.permutation(key_order, BATCH_ROWS)
    lengths = jax.random.randint(key_len, (BATCH_ROWS,), CACHE_LEN // 2, CACHE_LEN + 1)
    lengths = jnp.where(row_order == 0, CACHE_LEN, jnp.where(row_order == 1, CACHE_LEN // 2, lengths))
    return lengths.astype(jnp.int32)


def setup_inputs(seed: int = 0, part: int = 0) -> dict:
    shared_keys = jax.random.split(jax.random.key(seed), 9)
    own_keys = jax.random.split(jax.random.fold_in(jax.random.key(seed + 1), part), 4)
    q_width = Q_HEADS * HEAD_DIM
    kv_width = KV_HEADS * HEAD_DIM
    q_cols = jnp.repeat(head_scales(shared_keys[0], Q_HEADS, 0.5), HEAD_DIM)
    k_cols = jnp.repeat(head_scales(shared_keys[1], KV_HEADS, 0.5), HEAD_DIM)
    w_query = jax.random.normal(shared_keys[2], (MODEL_DIM, q_width), jnp.float32) * (MODEL_DIM ** -0.5) * q_cols[None, :]
    w_key = jax.random.normal(shared_keys[3], (MODEL_DIM, kv_width), jnp.float32) * (MODEL_DIM ** -0.5) * k_cols[None, :]
    w_value = jax.random.normal(shared_keys[4], (MODEL_DIM, kv_width), jnp.float32) * (MODEL_DIM ** -0.5)
    w_out = jax.random.normal(shared_keys[5], (q_width, MODEL_DIM), jnp.float32) * (q_width ** -0.5)
    q_gain = 1.0 + 0.25 * jax.random.normal(shared_keys[6], (q_width,), jnp.float32)
    k_gain = 1.0 + 0.25 * jax.random.normal(shared_keys[7], (kv_width,), jnp.float32)
    post_gain = 1.0 + 0.3 * jax.random.normal(shared_keys[8], (MODEL_DIM,), jnp.float32)
    prefix_len = draw_prefix(own_keys[0])
    x_chunk = jax.random.normal(own_keys[1], (BATCH_ROWS, CHUNK_LEN, MODEL_DIM), jnp.float32)
    stale_mask = jnp.arange(CACHE_LEN)[None, :] >= prefix_len[:, None]
    slot_scale = jnp.where(stale_mask, 3.0, 1.0)[:, :, None, None]
    cache_k = 0.8 * jax.random.normal(own_keys[2], (BATCH_ROWS, CACHE_LEN, KV_HEADS, HEAD_DIM), jnp.float32) * slot_scale
    cache_v = jax.random.normal(own_keys[3], (BATCH_ROWS, CACHE_LEN, KV_HEADS, HEAD_DIM), jnp.float32) * slot_scale
    return {
        'x_chunk': x_chunk.astype(jnp.bfloat16),
        'w_query': w_query.astype(jnp.bfloat16),
        'w_key': w_key.astype(jnp.bfloat16),
        'w_value': w_value.astype(jnp.bfloat16),
        'w_out': w_out.astype(jnp.bfloat16),
        'q_gain': q_gain.astype(jnp.bfloat16),
        'k_gain': k_gain.astype(jnp.bfloat16),
        'post_gain': post_gain.astype(jnp.bfloat16),
        'cache_k': cache_k.astype(jnp.bfloat16),
        'cache_v': cache_v.astype(jnp.bfloat16),
        'prefix_len': prefix_len,
    }


def rms_norm(raw_vals, gain_vec):
    mean_sq = jnp.mean(raw_vals * raw_vals, axis=-1, keepdims=True)
    return raw_vals * lax.rsqrt(mean_sq + NORM_EPS) * gain_vec.astype(jnp.float32)


def rope_apply(head_vals, positions):
    half_dim = HEAD_DIM // 2
    inv_freq = ROPE_BASE ** (-(jnp.arange(half_dim, dtype=jnp.float32) * 2.0 / HEAD_DIM))
    angles = positions.astype(jnp.float32)[..., None] * inv_freq
    cos_tab = jnp.cos(angles)[..., None, :]
    sin_tab = jnp.sin(angles)[..., None, :]
    first_half = head_vals[..., :half_dim]
    second_half = head_vals[..., half_dim:]
    return jnp.concatenate([first_half * cos_tab - second_half * sin_tab, second_half * cos_tab + first_half * sin_tab], axis=-1)


def reference(x_chunk, w_query, w_key, w_value, w_out, q_gain, k_gain, post_gain, cache_k, cache_v, prefix_len):
    groups = Q_HEADS // KV_HEADS
    tokens = x_chunk.reshape(BATCH_ROWS * CHUNK_LEN, MODEL_DIM)
    q_raw = jnp.dot(tokens, w_query, preferred_element_type=jnp.float32)
    k_raw = jnp.dot(tokens, w_key, preferred_element_type=jnp.float32)
    v_raw = jnp.dot(tokens, w_value, preferred_element_type=jnp.float32)
    positions = prefix_len[:, None] + jnp.arange(CHUNK_LEN, dtype=jnp.int32)[None, :]
    q_rot = rope_apply(rms_norm(q_raw, q_gain).reshape(BATCH_ROWS, CHUNK_LEN, Q_HEADS, HEAD_DIM), positions)
    k_rot = rope_apply(rms_norm(k_raw, k_gain).reshape(BATCH_ROWS, CHUNK_LEN, KV_HEADS, HEAD_DIM), positions)
    q_new = q_rot.astype(jnp.bfloat16).reshape(BATCH_ROWS, CHUNK_LEN, KV_HEADS, groups, HEAD_DIM)
    chunk_k = k_rot.astype(jnp.bfloat16)
    chunk_v = v_raw.astype(jnp.bfloat16).reshape(BATCH_ROWS, CHUNK_LEN, KV_HEADS, HEAD_DIM)
    key_index = jnp.arange(CACHE_LEN + CHUNK_LEN)
    score_scale = HEAD_DIM ** -0.5

    def row_attention(row_in):
        q_row, k_row, v_row, ck_row, cv_row, valid_len = row_in
        all_keys = jnp.concatenate([ck_row, k_row], axis=0).astype(jnp.float32)
        all_values = jnp.concatenate([cv_row, v_row], axis=0).astype(jnp.float32)
        q_blocks = q_row.reshape(CHUNK_LEN // QUERY_BLOCK, QUERY_BLOCK, KV_HEADS, groups, HEAD_DIM).astype(jnp.float32)

        def block_attention(block_in):
            q_blk, block_id = block_in
            q_index = block_id * QUERY_BLOCK + jnp.arange(QUERY_BLOCK)
            allowed = jnp.where(key_index[None, :] < CACHE_LEN, key_index[None, :] < valid_len, key_index[None, :] - CACHE_LEN <= q_index[:, None])
            scores = jnp.einsum('qkgd,tkd->qkgt', q_blk, all_keys) * score_scale
            scores = jnp.where(allowed[:, None, None, :], scores, -jnp.inf)
            probs_f = jax.nn.softmax(scores, axis=-1)
            return jnp.einsum('qkgt,tkd->qkgd', probs_f, all_values)

        blocks = lax.map(block_attention, (q_blocks, jnp.arange(CHUNK_LEN // QUERY_BLOCK)))
        return blocks.reshape(CHUNK_LEN, Q_HEADS * HEAD_DIM)

    attn_out = lax.map(row_attention, (q_new, chunk_k, chunk_v, cache_k, cache_v, prefix_len))
    attn_out = attn_out.astype(jnp.bfloat16).reshape(BATCH_ROWS * CHUNK_LEN, Q_HEADS * HEAD_DIM)
    mixed_sum = jnp.dot(attn_out, w_out, preferred_element_type=jnp.float32)
    result = x_chunk.astype(jnp.float32) + rms_norm(mixed_sum, post_gain).reshape(BATCH_ROWS, CHUNK_LEN, MODEL_DIM)
    return result.astype(jnp.bfloat16), chunk_k, chunk_v
```

```python
import functools
import math

import jax
import jax.numpy as jnp
from jax import lax
from jax.experimental import pallas as pl
from jax.experimental.pallas import tpu as pltpu
from jax.sharding import PartitionSpec as P

NORM_EPS = 1e-6
ROPE_BASE = 500000.0
MASK_VALUE = -1e30
ROW_CHUNKS = 3
QUERY_TILE = 256
TOKEN_TILE = 256
KEY_PIECE = 512
VMEM_BYTES = 60 * 1024 * 1024
MESH = pl.DeviceIdType.MESH


def rope_tables(positions, head_dim):
    half_dim = head_dim // 2
    inv_freq = ROPE_BASE ** (-(jnp.arange(half_dim, dtype=jnp.float32) * 2.0 / head_dim))
    angles = positions.astype(jnp.float32)[:, None] * inv_freq
    cos_tab, sin_tab = jnp.cos(angles), jnp.sin(angles)
    return jnp.concatenate([cos_tab, cos_tab], axis=-1), jnp.concatenate([-sin_tab, sin_tab], axis=-1)


def exchange_kernel(axis, size, combine, x_ref, out_ref, held, send_sem, recv_sem):
    me = lax.axis_index(axis)
    barrier = pltpu.get_barrier_semaphore()
    for step in range(1, size):
        pl.semaphore_signal(barrier, inc=1, device_id={axis: lax.rem(me + step, size)}, device_id_type=MESH)
    pl.semaphore_wait(barrier, size - 1)
    copies = []
    for step in range(1, size):
        copy = pltpu.make_async_remote_copy(
            src_ref=x_ref,
            dst_ref=held.at[me],
            send_sem=send_sem.at[step - 1],
            recv_sem=recv_sem.at[step - 1],
            device_id={axis: lax.rem(me + step, size)},
            device_id_type=MESH,
        )
        copy.start()
        copies.append(copy)
    held[me] = x_ref[...]
    for copy in copies:
        copy.wait()
    if combine == 'sum':
        total = held[0]
        for src in range(1, size):
            total = total + held[src]
        out_ref[...] = total
    else:
        top = held[0]
        for src in range(1, size):
            top = jnp.maximum(top, held[src])
        total = jnp.exp2(held[0] - top)
        for src in range(1, size):
            total = total + jnp.exp2(held[src] - top)
        out_ref[...] = top + jnp.log2(total)


def exchange(vals, axis, size, combine, collective_id):
    return pl.pallas_call(
        functools.partial(exchange_kernel, axis, size, combine),
        out_shape=jax.ShapeDtypeStruct(vals.shape, vals.dtype),
        in_specs=[pl.BlockSpec(memory_space=pltpu.VMEM)],
        out_specs=pl.BlockSpec(memory_space=pltpu.VMEM),
        scratch_shapes=[
            pltpu.VMEM((size,) + vals.shape, vals.dtype),
            pltpu.SemaphoreType.DMA((size - 1,)),
            pltpu.SemaphoreType.DMA((size - 1,)),
        ],
        compiler_params=pltpu.CompilerParams(collective_id=collective_id, has_side_effects=True),
        cost_estimate=pl.CostEstimate(flops=8_000_000, bytes_accessed=2 * vals.size * 4, transcendentals=0),
        name='exchange_' + axis,
    )(vals)


def rope_kernel(head_dim, q_ref, k_ref, q_inv, k_inv, q_gain, k_gain, cos_ref, sin_ref, q_out, k_out):
    cos_tab, sin_tab = cos_ref[...], sin_ref[...]
    for raw, inv, gain, out in ((q_ref, q_inv, q_gain, q_out), (k_ref, k_inv, k_gain, k_out)):
        scale = inv[...]
        for head in range(raw.shape[1] // head_dim):
            cols = slice(head * head_dim, (head + 1) * head_dim)
            vals = raw[:, cols] * scale * gain[:, cols]
            out[:, cols] = (vals * cos_tab + pltpu.roll(vals, head_dim // 2, 1) * sin_tab).astype(out.dtype)


def norm_rope(q_raw, k_raw, q_inv, k_inv, q_gain, k_gain, cos_tab, sin_tab, head_dim):
    tokens, q_width = q_raw.shape
    k_width = k_raw.shape[1]
    tile = math.gcd(tokens, TOKEN_TILE)
    by_token = lambda width: pl.BlockSpec((tile, width), lambda i: (i, 0))
    whole = lambda width: pl.BlockSpec((1, width), lambda i: (0, 0))
    return pl.pallas_call(
        functools.partial(rope_kernel, head_dim),
        grid=(tokens // tile,),
        out_shape=(jax.ShapeDtypeStruct(q_raw.shape, jnp.bfloat16), jax.ShapeDtypeStruct(k_raw.shape, jnp.bfloat16)),
        in_specs=[by_token(q_width), by_token(k_width), by_token(head_dim), by_token(head_dim), whole(q_width), whole(k_width), by_token(head_dim), by_token(head_dim)],
        out_specs=(by_token(q_width), by_token(k_width)),
        compiler_params=pltpu.CompilerParams(vmem_limit_bytes=VMEM_BYTES),
        cost_estimate=pl.CostEstimate(flops=tokens * q_width * 8, bytes_accessed=tokens * (q_width + k_width) * 6, transcendentals=0),
        name='norm_rope',
    )(q_raw, k_raw, q_inv, k_inv, q_gain, k_gain, cos_tab, sin_tab)


def attention_kernel(row0, groups, exp_scale, info, q_ref, k_ref, v_ref, kc_ref, vc_ref, num_ref, max_ref, lse_ref, vt_ref, s_even, s_odd):
    blocks, _, chunk_dev, _ = q_ref.shape
    cache_dev, head_dim = k_ref.shape[2], k_ref.shape[3]
    per_tile = QUERY_TILE // chunk_dev
    halves = blocks // per_tile
    valid = info[1 + row0 + pl.program_id(0)]
    key_base = info[0]
    tiles = groups * halves
    piece = math.gcd(cache_dev, KEY_PIECE)
    scratch = (s_even, s_odd)

    def q_tile(tile):
        group, half = divmod(tile, halves)
        block = q_ref[half * per_tile:(half + 1) * per_tile, 0, :, group * head_dim:(group + 1) * head_dim]
        return block.reshape(QUERY_TILE, head_dim)

    def scores(keys, q_vals):
        return lax.dot_general(keys, q_vals, (((1,), (1,)), ((), ())), preferred_element_type=jnp.float32)

    def fold(vals):
        return jnp.max(vals.reshape(vals.shape[0] // 8, 8, QUERY_TILE), axis=0)

    def chunk_scores(tile, q_vals):
        vals = scores(kc_ref[0], q_vals)
        key_index = key_base + lax.broadcasted_iota(jnp.int32, vals.shape, 0)
        query_index = (tile % halves) * QUERY_TILE + lax.broadcasted_iota(jnp.int32, vals.shape, 1)
        vals = jnp.where(key_index <= query_index, vals, MASK_VALUE)
        scratch[tile % 2][cache_dev:cache_dev + chunk_dev, :] = vals
        return fold(vals)

    def cache_scores(tile, q_vals, first, masked):
        vals = scores(k_ref[0, 0, first:first + piece, :], q_vals)
        if masked:
            slot = first + lax.broadcasted_iota(jnp.int32, vals.shape, 0)
            vals = jnp.where(slot < valid, vals, MASK_VALUE)
        scratch[tile % 2][first:first + piece, :] = vals
        return fold(vals)

    def weights(tile, first, size, top_scaled):
        probs = jnp.exp2(scratch[tile % 2][first:first + size, :] * exp_scale - top_scaled)
        return probs.astype(jnp.bfloat16), jnp.sum(probs.reshape(size // 8, 8, QUERY_TILE), axis=0)

    def run(masked, with_cache):
        firsts = range(0, cache_dev, piece) if with_cache else ()

        def first_scores(tile):
            q_vals = q_tile(tile)
            top = chunk_scores(tile, q_vals)
            for first in firsts:
                top = jnp.maximum(top, cache_scores(tile, q_vals, first, masked))
            return top

        top = first_scores(0)
        for tile in range(tiles):
            top_scaled = jnp.max(top, axis=0, keepdims=True) * exp_scale
            more = tile + 1 < tiles
            if more:
                q_next = q_tile(tile + 1)
                top = chunk_scores(tile + 1, q_next)
            probs, den = weights(tile, cache_dev, chunk_dev, top_scaled)
            num = lax.dot_general(vc_ref[0], probs, (((0,), (0,)), ((), ())), preferred_element_type=jnp.float32)
            for first in firsts:
                if more:
                    top = jnp.maximum(top, cache_scores(tile + 1, q_next, first, masked))
                probs, part = weights(tile, first, piece, top_scaled)
                den = den + part
                num = num + jnp.dot(vt_ref[:, first:first + piece], probs, preferred_element_type=jnp.float32)
            num_ref[0, 0, tile] = num
            max_ref[0, 0, tile:tile + 1, :] = top_scaled
            lse_ref[0, 0, tile:tile + 1, :] = top_scaled + jnp.log2(jnp.sum(den, axis=0, keepdims=True))

    max_ref[...] = jnp.zeros_like(max_ref)
    lse_ref[...] = jnp.zeros_like(lse_ref)

    @pl.when(valid > 0)
    def _():
        vt_ref[...] = v_ref[0, 0].T

    pl.when(valid >= cache_dev)(lambda: run(False, True))
    pl.when(jnp.logical_and(valid > 0, valid < cache_dev))(lambda: run(True, True))
    pl.when(valid <= 0)(lambda: run(False, False))


def attention(info, q_all, k_heads, v_heads, chunk_k, chunk_v, row0, groups):
    blocks, rows, chunk_dev, q_width = q_all.shape
    _, kv_local, cache_dev, head_dim = k_heads.shape
    tiles = groups * (blocks * chunk_dev // QUERY_TILE)
    pad = -(-tiles // 8) * 8
    q_head_width = q_width // kv_local
    stats = jax.ShapeDtypeStruct((rows, kv_local, pad, QUERY_TILE), jnp.float32)
    stats_spec = pl.BlockSpec((1, 1, pad, QUERY_TILE), lambda r, h, _: (r, h, 0, 0))
    scores = rows * q_width // head_dim * blocks * chunk_dev * (cache_dev + chunk_dev)
    return pl.pallas_call(
        functools.partial(attention_kernel, row0, groups, math.log2(math.e) * head_dim ** -0.5),
        out_shape=(jax.ShapeDtypeStruct((rows, kv_local, tiles, head_dim, QUERY_TILE), jnp.float32), stats, stats),
        grid_spec=pltpu.PrefetchScalarGridSpec(
            num_scalar_prefetch=1,
            grid=(rows, kv_local),
            in_specs=[
                pl.BlockSpec((blocks, 1, chunk_dev, q_head_width), lambda r, h, _: (0, r, 0, h)),
                pl.BlockSpec((1, 1, cache_dev, head_dim), lambda r, h, _: (row0 + r, h, 0, 0)),
                pl.BlockSpec((1, 1, cache_dev, head_dim), lambda r, h, _: (row0 + r, h, 0, 0)),
                pl.BlockSpec((1, chunk_dev, head_dim), lambda r, h, _: (row0 + r, 0, h)),
                pl.BlockSpec((1, chunk_dev, head_dim), lambda r, h, _: (row0 + r, 0, h)),
            ],
            out_specs=(pl.BlockSpec((1, 1, tiles, head_dim, QUERY_TILE), lambda r, h, _: (r, h, 0, 0, 0)), stats_spec, stats_spec),
            scratch_shapes=[
                pltpu.VMEM((head_dim, cache_dev), jnp.bfloat16),
                pltpu.VMEM((cache_dev + chunk_dev, QUERY_TILE), jnp.float32),
                pltpu.VMEM((cache_dev + chunk_dev, QUERY_TILE), jnp.float32),
            ],
        ),
        compiler_params=pltpu.CompilerParams(vmem_limit_bytes=VMEM_BYTES),
        cost_estimate=pl.CostEstimate(flops=scores * head_dim * 8, bytes_accessed=scores // 8, transcendentals=scores),
        name='attention',
    )(info, q_all, k_heads, v_heads, chunk_k, chunk_v)


def scale_kernel(num_ref, max_ref, lse_ref, out_ref):
    _, kv_local, tiles, head_dim, _ = num_ref.shape
    blocks, chunk_dev, _ = out_ref.shape
    halves = blocks * chunk_dev // QUERY_TILE
    groups = tiles // halves
    per_tile = QUERY_TILE // chunk_dev
    for kv_head in range(kv_local):
        factor = jnp.exp2(max_ref[0, kv_head] - lse_ref[0, kv_head])
        for group in range(groups):
            head = kv_head * groups + group
            for half in range(halves):
                at = group * halves + half
                scaled = (num_ref[0, kv_head, at] * factor[at:at + 1, :]).T
                out_ref[half * per_tile:(half + 1) * per_tile, :, head * head_dim:(head + 1) * head_dim] = scaled.reshape(per_tile, chunk_dev, head_dim)


def scale_parts(num, tops, lse, blocks, chunk_dev):
    rows, kv_local, tiles, head_dim, _ = num.shape
    pad = tops.shape[2]
    width = kv_local * tiles * QUERY_TILE // (blocks * chunk_dev) * head_dim
    stats_spec = pl.BlockSpec((1, kv_local, pad, QUERY_TILE), lambda r: (r, 0, 0, 0))
    return pl.pallas_call(
        scale_kernel,
        grid=(rows,),
        out_shape=jax.ShapeDtypeStruct((blocks, rows * chunk_dev, width), jnp.float32),
        in_specs=[pl.BlockSpec((1, kv_local, tiles, head_dim, QUERY_TILE), lambda r: (r, 0, 0, 0, 0)), stats_spec, stats_spec],
        out_specs=pl.BlockSpec((blocks, chunk_dev, width), lambda r: (0, r, 0)),
        compiler_params=pltpu.CompilerParams(vmem_limit_bytes=VMEM_BYTES),
        cost_estimate=pl.CostEstimate(flops=num.size * 2, bytes_accessed=num.size * 8, transcendentals=0),
        name='scale_parts',
    )(num, tops, lse)


def out_kernel(tp_size, first, info, *refs):
    o_ref, w_ref, x_ref, gain_ref = refs[:4]
    out_ref = refs[-1]
    me = info[0]
    total = None
    for src in range(tp_size):
        part = jnp.dot(o_ref[lax.rem(src - me + tp_size, tp_size)], w_ref[src], preferred_element_type=jnp.float32)
        total = part if total is None else total + part
    normed = total * lax.rsqrt(jnp.mean(total * total, axis=-1, keepdims=True) + NORM_EPS) * gain_ref[...]
    out_ref[...] = (x_ref[...].astype(jnp.float32) + normed).astype(out_ref.dtype)


def project_out(info, o_all, w_full, x_tokens, gain, earlier, token0):
    tp_size, tokens, width = o_all.shape
    model_dim = x_tokens.shape[1]
    tile = math.gcd(tokens, TOKEN_TILE)
    shift = token0 // tile
    here = lambda i, _: (shift + i, 0)
    in_specs = [
        pl.BlockSpec((tp_size, tile, width), lambda i, _: (0, i, 0)),
        pl.BlockSpec((tp_size, width, model_dim), lambda i, _: (0, 0, 0), pipeline_mode=pl.Buffered(1)),
        pl.BlockSpec((tile, model_dim), here),
        pl.BlockSpec((1, model_dim), lambda i, _: (0, 0)),
    ]
    operands = [info, o_all, w_full, x_tokens, gain]
    aliases = {}
    if earlier is not None:
        in_specs.append(pl.BlockSpec(memory_space=pl.ANY))
        operands.append(earlier)
        aliases = {5: 0}
    return pl.pallas_call(
        functools.partial(out_kernel, tp_size, earlier is None),
        out_shape=jax.ShapeDtypeStruct(x_tokens.shape, jnp.bfloat16),
        grid_spec=pltpu.PrefetchScalarGridSpec(
            num_scalar_prefetch=1,
            grid=(tokens // tile,),
            in_specs=in_specs,
            out_specs=pl.BlockSpec((tile, model_dim), here),
        ),
        input_output_aliases=aliases,
        compiler_params=pltpu.CompilerParams(vmem_limit_bytes=VMEM_BYTES),
        cost_estimate=pl.CostEstimate(flops=2 * tokens * tp_size * width * model_dim, bytes_accessed=2 * w_full.size, transcendentals=0),
        name='project_out',
    )(*operands)


def gather_by_distance(vals, axis, size):
    up = [(i, (i + 1) % size) for i in range(size)]
    down = [(i, (i - 1) % size) for i in range(size)]
    if size != 4:
        steps = [vals]
        for _ in range(size - 1):
            steps.append(lax.ppermute(steps[-1], axis, down))
        return jnp.stack(steps)
    mid = vals.shape[0] // 2
    below = lax.ppermute(vals, axis, up)
    above = lax.ppermute(vals, axis, down)
    far_low = lax.ppermute(below[:mid], axis, up)
    far_high = lax.ppermute(above[mid:], axis, down)
    return jnp.stack([vals, above, jnp.concatenate([far_low, far_high]), below])


def solution(mesh):
    cp_size = mesh.shape['cp']
    tp_size = mesh.shape['tp']

    def local_step(x_chunk, w_query, w_key, w_value, w_out, q_gain, k_gain, post_gain, cache_k, cache_v, prefix_len):
        batch_rows, chunk_dev, model_dim = x_chunk.shape
        cache_dev, kv_local, head_dim = cache_k.shape[1:]
        q_width, k_width = w_query.shape[1], w_key.shape[1]
        groups = q_width // k_width
        cp_index = lax.axis_index('cp')
        tp_index = lax.axis_index('tp')
        rows = batch_rows // ROW_CHUNKS
        tokens = x_chunk.reshape(batch_rows * chunk_dev, model_dim)

        w_piece = w_out.shape[0] // cp_size
        w_own = lax.dynamic_slice_in_dim(w_out, cp_index * w_piece, w_piece, axis=0)
        w_full = lax.all_gather(w_own, ('tp', 'cp'), axis=0, tiled=True).reshape(tp_size, q_width, model_dim)

        q_raw = jnp.dot(tokens, w_query, preferred_element_type=jnp.float32)
        k_raw = jnp.dot(tokens, w_key, preferred_element_type=jnp.float32)
        chunk_v = jnp.dot(tokens, w_value, preferred_element_type=jnp.float32).astype(jnp.bfloat16)
        squares = jnp.stack([jnp.sum(q_raw * q_raw, axis=-1), jnp.sum(k_raw * k_raw, axis=-1)])
        square_sums = exchange(squares.reshape(-1, 128), 'tp', tp_size, 'sum', 0).reshape(squares.shape)
        q_inv = lax.rsqrt(square_sums[0] / (q_width * tp_size) + NORM_EPS)
        k_inv = lax.rsqrt(square_sums[1] / (k_width * tp_size) + NORM_EPS)
        wide = lambda vec: jnp.broadcast_to(vec[:, None], (vec.shape[0], head_dim))
        positions = (prefix_len[:, None] + cp_index * chunk_dev + jnp.arange(chunk_dev, dtype=jnp.int32)[None, :]).reshape(-1)
        cos_tab, sin_tab = rope_tables(positions, head_dim)
        q_new, chunk_k = norm_rope(
            q_raw, k_raw, wide(q_inv), wide(k_inv), q_gain.astype(jnp.float32)[None, :], k_gain.astype(jnp.float32)[None, :], cos_tab, sin_tab, head_dim
        )
        q_new, w_full = lax.optimization_barrier((q_new, w_full))
        q_new = q_new.reshape(batch_rows, chunk_dev, q_width)
        k_rows = chunk_k.reshape(batch_rows, chunk_dev, k_width)
        v_rows = chunk_v.reshape(batch_rows, chunk_dev, k_width)
        k_heads = jnp.transpose(cache_k, (0, 2, 1, 3))
        v_heads = jnp.transpose(cache_v, (0, 2, 1, 3))
        valid = jnp.clip(prefix_len - cp_index * cache_dev, 0, cache_dev)
        info = jnp.concatenate([jnp.reshape(cp_index * chunk_dev, (1,)), valid]).astype(jnp.int32)
        tp_info = jnp.reshape(tp_index, (1,)).astype(jnp.int32)
        post = post_gain.astype(jnp.float32)[None, :]

        gathered = [lax.all_gather(q_new[c * rows:(c + 1) * rows], 'cp', axis=0, tiled=False) for c in range(ROW_CHUNKS)]
        parts = []
        for c in range(ROW_CHUNKS):
            num, tops, lse = attention(info, gathered[c], k_heads, v_heads, k_rows, v_rows, c * rows, groups)
            lse_all = exchange(lse.reshape(-1, QUERY_TILE), 'cp', cp_size, 'lse', 1 + c).reshape(lse.shape)
            scaled = scale_parts(num, tops, lse_all, cp_size, chunk_dev)
            parts.append(lax.psum_scatter(scaled, 'cp', scatter_dimension=0, tiled=False))
        block_out = None
        for c in range(ROW_CHUNKS):
            part = parts[c]
            if c:
                part, block_out = lax.optimization_barrier((part, block_out))
            o_all = gather_by_distance(part.astype(jnp.bfloat16), 'tp', tp_size)
            block_out = project_out(tp_info, o_all, w_full, tokens, post, block_out, c * rows * chunk_dev)
        heads_shape = (batch_rows, chunk_dev, kv_local, head_dim)
        return block_out.reshape(x_chunk.shape), chunk_k.reshape(heads_shape), chunk_v.reshape(heads_shape)

    x_spec = P('dp', 'cp', None)
    head_spec = P('dp', 'cp', 'tp', None)
    in_specs = (x_spec, P(None, 'tp'), P(None, 'tp'), P(None, 'tp'), P('tp', None), P('tp'), P('tp'), P(None), head_spec, head_spec, P('dp'))
    out_specs = (x_spec, head_spec, head_spec)
    return jax.shard_map(local_step, mesh=mesh, in_specs=in_specs, out_specs=out_specs, check_vma=False)
```

```python
import functools
import math

import jax
import jax.numpy as jnp
from jax import lax
from jax.experimental import pallas as pl
from jax.experimental.pallas import tpu as pltpu
from jax.sharding import PartitionSpec as P


NORM_EPS = 1e-6
ROPE_BASE = 500000.0
MASK_VALUE = -(2.0 ** 100)
ROW_CHUNKS = 3
TOKEN_TILE = 256
KEY_PIECE = 512
CORES = 2
SWAP_AT = 2
VMEM_BYTES = 60 * 1024 * 1024
MESH = pl.DeviceIdType.MESH


def rope_tables(positions, head_dim):
    half_dim = head_dim // 2
    inv_freq = ROPE_BASE ** (-(jnp.arange(half_dim, dtype=jnp.float32) * 2.0 / head_dim))
    angles = positions.astype(jnp.float32)[:, None] * inv_freq
    cos_tab, sin_tab = jnp.cos(angles), jnp.sin(angles)
    return jnp.concatenate([cos_tab, cos_tab], axis=-1), jnp.concatenate([-sin_tab, sin_tab], axis=-1)


def exchange_kernel(axis, size, stride, combine, x_ref, out_ref, held, send_sem, recv_sem):
    me = lax.axis_index(axis)
    slot = me // stride
    peers = [lax.rem(me + step * stride, size * stride) for step in range(1, size)]
    barrier = pltpu.get_barrier_semaphore()
    for peer in peers:
        pl.semaphore_signal(barrier, inc=1, device_id={axis: peer}, device_id_type=MESH)
    pl.semaphore_wait(barrier, size - 1)
    copies = []
    for at, peer in enumerate(peers):
        copy = pltpu.make_async_remote_copy(
            src_ref=x_ref,
            dst_ref=held.at[slot],
            send_sem=send_sem.at[at],
            recv_sem=recv_sem.at[at],
            device_id={axis: peer},
            device_id_type=MESH,
        )
        copy.start()
        copies.append(copy)
    held[slot] = x_ref[...]
    for copy in copies:
        copy.wait()
    if combine == 'sum':
        total = held[0]
        for src in range(1, size):
            total = total + held[src]
        out_ref[...] = total
    else:
        top = held[0]
        for src in range(1, size):
            top = jnp.maximum(top, held[src])
        total = jnp.exp2(held[0] - top)
        for src in range(1, size):
            total = total + jnp.exp2(held[src] - top)
        out_ref[...] = top + jnp.log2(total)


def exchange(vals, axis, size, stride, combine, collective_id):
    return pl.pallas_call(
        functools.partial(exchange_kernel, axis, size, stride, combine),
        out_shape=jax.ShapeDtypeStruct(vals.shape, vals.dtype),
        in_specs=[pl.BlockSpec(memory_space=pltpu.VMEM)],
        out_specs=pl.BlockSpec(memory_space=pltpu.VMEM),
        scratch_shapes=[
            pltpu.VMEM((size,) + vals.shape, vals.dtype),
            pltpu.SemaphoreType.DMA((size - 1,)),
            pltpu.SemaphoreType.DMA((size - 1,)),
        ],
        compiler_params=pltpu.CompilerParams(collective_id=collective_id, has_side_effects=True),
        cost_estimate=pl.CostEstimate(flops=8_000_000, bytes_accessed=2 * vals.size * 4, transcendentals=0),
    )(vals)


def rope_kernel(head_dim, q_ref, k_ref, q_inv, k_inv, q_gain, k_gain, cos_ref, sin_ref, q_out, k_out):
    cos_tab, sin_tab = cos_ref[...], sin_ref[...]
    for raw, inv, gain, out in ((q_ref, q_inv, q_gain, q_out), (k_ref, k_inv, k_gain, k_out)):
        scale = inv[...]
        for head in range(raw.shape[1] // head_dim):
            cols = slice(head * head_dim, (head + 1) * head_dim)
            vals = raw[:, cols] * scale * gain[:, cols]
            out[:, cols] = (vals * cos_tab + pltpu.roll(vals, head_dim // 2, 1) * sin_tab).astype(out.dtype)


def norm_rope(q_raw, k_raw, q_inv, k_inv, q_gain, k_gain, cos_tab, sin_tab, head_dim):
    tokens, q_width = q_raw.shape
    k_width = k_raw.shape[1]
    tile = math.gcd(tokens, TOKEN_TILE)
    by_token = lambda width: pl.BlockSpec((tile, width), lambda i: (i, 0))
    whole = lambda width: pl.BlockSpec((1, width), lambda i: (0, 0))
    return pl.pallas_call(
        functools.partial(rope_kernel, head_dim),
        grid=(tokens // tile,),
        out_shape=(jax.ShapeDtypeStruct(q_raw.shape, jnp.bfloat16), jax.ShapeDtypeStruct(k_raw.shape, jnp.bfloat16)),
        in_specs=[by_token(q_width), by_token(k_width), by_token(head_dim), by_token(head_dim), whole(q_width), whole(k_width), by_token(head_dim), by_token(head_dim)],
        out_specs=(by_token(q_width), by_token(k_width)),
        compiler_params=pltpu.CompilerParams(vmem_limit_bytes=VMEM_BYTES),
        cost_estimate=pl.CostEstimate(flops=tokens * q_width * 8, bytes_accessed=tokens * (q_width + k_width) * 6, transcendentals=0),
        name='norm_rope',
    )(q_raw, k_raw, q_inv, k_inv, q_gain, k_gain, cos_tab, sin_tab)


def attention_kernel(row0, groups, exp_scale, info, q_ref, k_ref, v_ref, kc_ref, vc_ref, own_ref, other_ref, stats_ref, vt_ref, s_even, s_odd):
    blocks, _, chunk_dev, _ = q_ref.shape
    cache_dev, head_dim = k_ref.shape[2], k_ref.shape[3]
    core = lax.rem(info[0], CORES)
    key_base = info[0] * chunk_dev
    valid = info[1 + row0 + pl.program_id(0)]
    tiles = groups * CORES
    q_size = blocks // CORES * chunk_dev
    piece = math.gcd(cache_dev, KEY_PIECE)
    scratch = (s_even, s_odd)

    def q_tile(tile):
        side, group = divmod(tile, groups)
        first = lax.rem(core + side, CORES)
        cols = slice(group * head_dim, (group + 1) * head_dim)
        return jnp.concatenate([q_ref[first + step, 0, :, cols] for step in range(0, blocks, CORES)], axis=0)

    def scores(keys, q_vals):
        return lax.dot_general(keys, q_vals, (((1,), (1,)), ((), ())), preferred_element_type=jnp.float32)

    def fold(vals):
        return jnp.max(vals.reshape(vals.shape[0] // 8, 8, q_size), axis=0)

    def chunk_scores(tile, q_vals):
        vals = scores(kc_ref[0], q_vals)
        key_index = key_base + lax.broadcasted_iota(jnp.int32, vals.shape, 0)
        lane = lax.broadcasted_iota(jnp.int32, vals.shape, 1)
        block = (lane // chunk_dev) * CORES + lax.rem(core + tile // groups, CORES)
        query_index = block * chunk_dev + lane % chunk_dev
        vals = jnp.where(key_index <= query_index, vals, MASK_VALUE)
        scratch[tile % 2][cache_dev:cache_dev + chunk_dev, :] = vals
        return fold(vals)

    def cache_scores(tile, q_vals, first, masked):
        vals = scores(k_ref[0, 0, first:first + piece, :], q_vals)
        if masked:
            slot = first + lax.broadcasted_iota(jnp.int32, vals.shape, 0)
            vals = jnp.where(slot < valid, vals, MASK_VALUE)
        scratch[tile % 2][first:first + piece, :] = vals
        return fold(vals)

    def weights(tile, first, size, top_scaled):
        probs = jnp.exp2(scratch[tile % 2][first:first + size, :] * exp_scale - top_scaled)
        return probs.astype(jnp.bfloat16), jnp.sum(probs.reshape(size // 8, 8, q_size), axis=0)

    def run(masked, with_cache):
        firsts = range(0, cache_dev, piece) if with_cache else ()

        def first_scores(tile):
            q_vals = q_tile(tile)
            top = chunk_scores(tile, q_vals)
            for first in firsts:
                top = jnp.maximum(top, cache_scores(tile, q_vals, first, masked))
            return top

        top = first_scores(0)
        for tile in range(tiles):
            top_scaled = jnp.max(top, axis=0, keepdims=True) * exp_scale
            more = tile + 1 < tiles
            if more:
                q_next = q_tile(tile + 1)
                top = chunk_scores(tile + 1, q_next)
            probs, den = weights(tile, cache_dev, chunk_dev, top_scaled)
            num = lax.dot_general(vc_ref[0], probs, (((0,), (0,)), ((), ())), preferred_element_type=jnp.float32)
            for first in firsts:
                if more:
                    top = jnp.maximum(top, cache_scores(tile + 1, q_next, first, masked))
                probs, part = weights(tile, first, piece, top_scaled)
                den = den + part
                num = num + jnp.dot(vt_ref[:, first:first + piece], probs, preferred_element_type=jnp.float32)
            (own_ref, other_ref)[tile // groups][0, 0, tile % groups] = num
            stats_ref[0, 0, tile:tile + 1, :] = top_scaled
            stats_ref[0, 0, tiles + tile:tiles + tile + 1, :] = top_scaled + jnp.log2(jnp.sum(den, axis=0, keepdims=True))

    @pl.when(valid > 0)
    def _():
        vt_ref[...] = v_ref[0, 0].T

    pl.when(valid >= cache_dev)(lambda: run(False, True))
    pl.when(jnp.logical_and(valid > 0, valid < cache_dev))(lambda: run(True, True))
    pl.when(valid <= 0)(lambda: run(False, False))


def attention(info, q_all, k_heads, v_heads, chunk_k, chunk_v, row0, groups):
    blocks, rows, chunk_dev, q_width = q_all.shape
    _, kv_local, cache_dev, head_dim = k_heads.shape
    q_size = blocks // CORES * chunk_dev
    q_head_width = q_width // kv_local
    num = jax.ShapeDtypeStruct((rows, kv_local, groups, head_dim, q_size), jnp.float32)
    num_spec = pl.BlockSpec((1, 1, groups, head_dim, q_size), lambda r, h, _: (r, h, 0, 0, 0))
    stats_rows = 2 * CORES * groups
    cache_spec = pl.BlockSpec((1, 1, cache_dev, head_dim), lambda r, h, _: (row0 + r, h, 0, 0))
    chunk_spec = pl.BlockSpec((1, chunk_dev, head_dim), lambda r, h, _: (row0 + r, 0, h))
    scores = rows * q_width // head_dim * blocks * chunk_dev * (cache_dev + chunk_dev)
    return pl.pallas_call(
        functools.partial(attention_kernel, row0, groups, math.log2(math.e) * head_dim ** -0.5),
        out_shape=(num, num, jax.ShapeDtypeStruct((rows, kv_local, stats_rows, q_size), jnp.float32)),
        grid_spec=pltpu.PrefetchScalarGridSpec(
            num_scalar_prefetch=1,
            grid=(rows, kv_local),
            in_specs=[
                pl.BlockSpec((blocks, 1, chunk_dev, q_head_width), lambda r, h, _: (0, r, 0, h)),
                cache_spec, cache_spec, chunk_spec, chunk_spec,
            ],
            out_specs=(num_spec, num_spec, pl.BlockSpec((1, 1, stats_rows, q_size), lambda r, h, _: (r, h, 0, 0))),
            scratch_shapes=[
                pltpu.VMEM((head_dim, cache_dev), jnp.bfloat16),
                pltpu.VMEM((cache_dev + chunk_dev, q_size), jnp.float32),
                pltpu.VMEM((cache_dev + chunk_dev, q_size), jnp.float32),
            ],
        ),
        compiler_params=pltpu.CompilerParams(vmem_limit_bytes=VMEM_BYTES),
        cost_estimate=pl.CostEstimate(flops=1_000_000, bytes_accessed=scores // 8, transcendentals=0),
        name='attention',
    )(info, q_all, k_heads, v_heads, chunk_k, chunk_v)


def merge_kernel(own_ref, peer_ref, own_stats, peer_stats, lse_ref, out_ref):
    _, kv_local, groups, head_dim, _ = own_ref.shape
    blocks, chunk_dev, _ = out_ref.shape
    for kv_head in range(kv_local):
        lse = lse_ref[0, kv_head]
        own_factor = jnp.exp2(own_stats[0, kv_head, :groups] - lse)
        peer_factor = jnp.exp2(peer_stats[0, kv_head, groups:2 * groups] - lse)
        for group in range(groups):
            head = kv_head * groups + group
            at = slice(group, group + 1)
            both = own_ref[0, kv_head, group] * own_factor[at] + peer_ref[0, kv_head, group] * peer_factor[at]
            out_ref[:, :, head * head_dim:(head + 1) * head_dim] = both.T.reshape(blocks, chunk_dev, head_dim)


def merge_parts(own, peer, own_stats, peer_stats, lse, chunk_dev):
    rows, kv_local, groups, head_dim, q_size = own.shape
    blocks = q_size // chunk_dev
    width = kv_local * groups * head_dim
    by_row = lambda shape: pl.BlockSpec((1,) + shape[1:], lambda r: (r,) + (0,) * (len(shape) - 1))
    return pl.pallas_call(
        merge_kernel,
        grid=(rows,),
        out_shape=jax.ShapeDtypeStruct((blocks, rows * chunk_dev, width), jnp.float32),
        in_specs=[by_row(own.shape), by_row(own.shape), by_row(own_stats.shape), by_row(own_stats.shape), by_row(lse.shape)],
        out_specs=pl.BlockSpec((blocks, chunk_dev, width), lambda r: (0, r, 0)),
        compiler_params=pltpu.CompilerParams(vmem_limit_bytes=VMEM_BYTES),
        cost_estimate=pl.CostEstimate(flops=own.size * 8, bytes_accessed=own.size * 12, transcendentals=0),
        name='merge_parts',
    )(own, peer, own_stats, peer_stats, lse)


def out_kernel(tp_size, *refs):
    info = refs[0]
    w_refs, o_refs = refs[1:1 + 2 * tp_size - 1], refs[2 * tp_size:2 * tp_size + tp_size + 1]
    x_ref, gain_ref = refs[3 * tp_size + 1:3 * tp_size + 3]
    out_ref, w_held, o_held, w_sem, o_sem = refs[-5:]
    me, core = info[0], info[1]
    w_half = w_held.shape[1] // CORES
    o_half = o_held.shape[1] // 2
    tile = x_ref.shape[0]
    step = pl.program_id(0)

    @pl.when(step == 0)
    def _():
        for away in range(tp_size):
            slot = lax.rem(me + away, tp_size)
            if away == tp_size // 2:
                for part in range(2):
                    pltpu.make_async_copy(o_refs[away + part], o_held.at[slot, pl.ds(part * o_half, o_half)], o_sem.at[slot]).start()
            else:
                pltpu.make_async_copy(o_refs[away + (away > tp_size // 2)], o_held.at[slot], o_sem.at[slot]).start()
        for away in range(tp_size):
            slot = lax.rem(me + away, tp_size)
            if away == 0:
                pltpu.make_async_copy(w_refs[0], w_held.at[slot], w_sem.at[slot]).start()
            else:
                for part in range(CORES):
                    first = pl.multiple_of(lax.rem(core + part, CORES) * w_half, 8)
                    pltpu.make_async_copy(w_refs[CORES * away - 1 + part], w_held.at[slot, pl.ds(first, w_half)], w_sem.at[slot]).start()

    total = None
    for src in range(tp_size):
        @pl.when(step == 0)
        def _():
            pltpu.make_async_copy(o_held.at[src], o_held.at[src], o_sem.at[src]).wait()
            pltpu.make_async_copy(w_held.at[src], w_held.at[src], w_sem.at[src]).wait()

        part = jnp.dot(o_held[src, pl.ds(pl.multiple_of(step * tile, tile), tile), :], w_held[src], preferred_element_type=jnp.float32)
        total = part if total is None else total + part
    normed = total * lax.rsqrt(jnp.mean(total * total, axis=-1, keepdims=True) + NORM_EPS) * gain_ref[...]
    out_ref[...] = (x_ref[...].astype(jnp.float32) + normed).astype(out_ref.dtype)


def project_out(info, w_parts, o_parts, x_tokens, gain, earlier, token0):
    tp_size = (len(w_parts) + 1) // CORES
    tokens, width = o_parts[0].shape
    model_dim = x_tokens.shape[1]
    tile = math.gcd(tokens, TOKEN_TILE)
    shift = token0 // tile
    here = lambda i, _: (shift + i, 0)
    in_hbm = pl.BlockSpec(memory_space=pl.ANY)
    in_specs = [in_hbm] * (len(w_parts) + len(o_parts)) + [pl.BlockSpec((tile, model_dim), here), pl.BlockSpec((1, model_dim), lambda i, _: (0, 0))]
    operands = [info, *w_parts, *o_parts, x_tokens, gain]
    aliases = {}
    if earlier is not None:
        in_specs.append(in_hbm)
        aliases = {len(operands): 0}
        operands.append(earlier)
    return pl.pallas_call(
        functools.partial(out_kernel, tp_size),
        out_shape=jax.ShapeDtypeStruct(x_tokens.shape, jnp.bfloat16),
        grid_spec=pltpu.PrefetchScalarGridSpec(
            num_scalar_prefetch=1,
            grid=(tokens // tile,),
            in_specs=in_specs,
            out_specs=pl.BlockSpec((tile, model_dim), here),
            scratch_shapes=[
                pltpu.VMEM((tp_size, width, model_dim), jnp.bfloat16),
                pltpu.VMEM((tp_size, tokens, width), jnp.bfloat16),
                pltpu.SemaphoreType.DMA((tp_size,)),
                pltpu.SemaphoreType.DMA((tp_size,)),
            ],
        ),
        input_output_aliases=aliases,
        compiler_params=pltpu.CompilerParams(vmem_limit_bytes=VMEM_BYTES),
        cost_estimate=pl.CostEstimate(flops=2 * tokens * tp_size * width * model_dim, bytes_accessed=8 * width * model_dim, transcendentals=0),
        name='project_out',
    )(*operands)


def ring(size, shift):
    return [(i, (i + shift) % size) for i in range(size)]


def gather_by_distance(vals, axis, size):
    mid = vals.shape[0] // 2
    below = lax.ppermute(vals, axis, ring(size, 1))
    above = lax.ppermute(vals, axis, ring(size, -1))
    far_low = lax.ppermute(below[:mid], axis, ring(size, 1))
    far_high = lax.ppermute(above[mid:], axis, ring(size, -1))
    return [vals, above, far_low, far_high, below]


def solution(mesh):
    cp_size = mesh.shape['cp']
    tp_size = mesh.shape['tp']

    def sublayer(x_chunk, w_query, w_key, w_value, w_out, q_gain, k_gain, post_gain, cache_k, cache_v, prefix_len):
        batch_rows, chunk_dev, model_dim = x_chunk.shape
        cache_dev, kv_local, head_dim = cache_k.shape[1:]
        q_width, k_width = w_query.shape[1], w_key.shape[1]
        groups = q_width // k_width
        cp_index = lax.axis_index('cp')
        tp_index = lax.axis_index('tp')
        rows = batch_rows // ROW_CHUNKS
        tokens = x_chunk.reshape(batch_rows * chunk_dev, model_dim)

        core_index = cp_index % CORES
        w_piece = w_out.shape[0] // CORES
        w_own = lax.dynamic_slice_in_dim(w_out, core_index * w_piece, w_piece, axis=0)
        w_mine = [lax.ppermute(w_own, 'tp', ring(tp_size, -away)) for away in range(1, tp_size)]
        partner = [(i, i + 1 - 2 * (i % CORES)) for i in range(cp_size)]
        same_core = [list(range(core, cp_size, CORES)) for core in range(CORES)]

        q_raw = jnp.dot(tokens, w_query, preferred_element_type=jnp.float32)
        q_squares = jnp.sum(q_raw * q_raw, axis=-1)
        k_raw = jnp.dot(tokens, w_key, preferred_element_type=jnp.float32)
        chunk_v = jnp.dot(tokens, w_value, preferred_element_type=jnp.float32).astype(jnp.bfloat16)
        squares = jnp.stack([q_squares, jnp.sum(k_raw * k_raw, axis=-1)])
        square_sums = exchange(squares.reshape(-1, 128), 'tp', tp_size, 1, 'sum', 0).reshape(squares.shape)
        q_inv = lax.rsqrt(square_sums[0] / (q_width * tp_size) + NORM_EPS)
        k_inv = lax.rsqrt(square_sums[1] / (k_width * tp_size) + NORM_EPS)
        wide = lambda vec: jnp.broadcast_to(vec[:, None], (vec.shape[0], head_dim))
        positions = (prefix_len[:, None] + cp_index * chunk_dev + jnp.arange(chunk_dev, dtype=jnp.int32)[None, :]).reshape(-1)
        cos_tab, sin_tab = rope_tables(positions, head_dim)
        q_new, chunk_k = norm_rope(
            q_raw, k_raw, wide(q_inv), wide(k_inv), q_gain.astype(jnp.float32)[None, :], k_gain.astype(jnp.float32)[None, :], cos_tab, sin_tab, head_dim
        )
        q_new = q_new.reshape(batch_rows, chunk_dev, q_width)
        k_rows = chunk_k.reshape(batch_rows, chunk_dev, k_width)
        v_rows = chunk_v.reshape(batch_rows, chunk_dev, k_width)
        k_heads = jnp.transpose(cache_k, (0, 2, 1, 3))
        v_heads = jnp.transpose(cache_v, (0, 2, 1, 3))
        valid = jnp.clip(prefix_len - cp_index * cache_dev, 0, cache_dev)
        info = jnp.concatenate([jnp.reshape(cp_index, (1,)), valid]).astype(jnp.int32)
        tp_info = jnp.stack([tp_index, core_index]).astype(jnp.int32)
        post = post_gain.astype(jnp.float32)[None, :]

        gathered = [lax.all_gather(q_new[c * rows:(c + 1) * rows], 'cp', axis=0, tiled=False) for c in range(ROW_CHUNKS)]
        parts = []
        for c in range(ROW_CHUNKS):
            own, other, stats = attention(info, gathered[c], k_heads, v_heads, k_rows, v_rows, c * rows, groups)
            if c == SWAP_AT:
                w_mine, other = lax.optimization_barrier((w_mine, other))
                w_theirs = [lax.ppermute(piece, 'cp', partner) for piece in w_mine]
                w_parts = [w_out] + [piece for pair in zip(w_mine, w_theirs) for piece in pair]
            peer = lax.ppermute(other, 'cp', partner)
            peer_stats = lax.ppermute(stats, 'cp', partner)
            own_lse, peer_lse = stats[:, :, 2 * groups:3 * groups], peer_stats[:, :, 3 * groups:]
            top = jnp.maximum(own_lse, peer_lse)
            pair_lse = top + jnp.log2(jnp.exp2(own_lse - top) + jnp.exp2(peer_lse - top))
            lse = exchange(pair_lse.reshape(-1, pair_lse.shape[-1]), 'cp', cp_size // CORES, CORES, 'lse', 1 + c).reshape(pair_lse.shape)
            merged = merge_parts(own, peer, stats, peer_stats, lse, chunk_dev)
            parts.append(lax.psum_scatter(merged, 'cp', scatter_dimension=0, axis_index_groups=same_core, tiled=False))
        block_out = None
        for c in range(ROW_CHUNKS):
            part = parts[c]
            if c:
                part, block_out = lax.optimization_barrier((part, block_out))
            o_parts = gather_by_distance(part.astype(jnp.bfloat16), 'tp', tp_size)
            block_out = project_out(tp_info, w_parts, o_parts, tokens, post, block_out, c * rows * chunk_dev)
        heads_shape = (batch_rows, chunk_dev, kv_local, head_dim)
        return block_out.reshape(x_chunk.shape), chunk_k.reshape(heads_shape), chunk_v.reshape(heads_shape)

    x_spec = P('dp', 'cp', None)
    head_spec = P('dp', 'cp', 'tp', None)
    in_specs = (x_spec, P(None, 'tp'), P(None, 'tp'), P(None, 'tp'), P('tp', None), P('tp'), P('tp'), P(None), head_spec, head_spec, P('dp'))
    out_specs = (x_spec, head_spec, head_spec)
    return jax.shard_map(sublayer, mesh=mesh, in_specs=in_specs, out_specs=out_specs, check_vma=False)
```

```python
import functools
import math

import jax
import jax.numpy as jnp
from jax import lax
from jax.experimental import pallas as pl
from jax.experimental.pallas import tpu as pltpu
from jax.sharding import PartitionSpec as P


NORM_EPS = 1e-6
ROPE_BASE = 500000.0
MASK_VALUE = -(2.0 ** 100)
ROW_CHUNKS = 3
TOKEN_TILE = 256
KEY_PIECE = 512
CORES = 2
SWAP_AT = 1
VMEM_BYTES = 60 * 1024 * 1024
MESH = pl.DeviceIdType.MESH


def rope_tables(positions, head_dim):
    half_dim = head_dim // 2
    inv_freq = ROPE_BASE ** (-(jnp.arange(half_dim, dtype=jnp.float32) * 2.0 / head_dim))
    angles = positions.astype(jnp.float32)[:, None] * inv_freq
    cos_tab, sin_tab = jnp.cos(angles), jnp.sin(angles)
    return jnp.concatenate([cos_tab, cos_tab], axis=-1), jnp.concatenate([-sin_tab, sin_tab], axis=-1)


def exchange_kernel(axis, size, stride, combine, x_ref, out_ref, held, send_sem, recv_sem):
    me = lax.axis_index(axis)
    slot = me // stride
    peers = [lax.rem(me + step * stride, size * stride) for step in range(1, size)]
    barrier = pltpu.get_barrier_semaphore()
    for peer in peers:
        pl.semaphore_signal(barrier, inc=1, device_id={axis: peer}, device_id_type=MESH)
    pl.semaphore_wait(barrier, size - 1)
    copies = []
    for at, peer in enumerate(peers):
        copy = pltpu.make_async_remote_copy(
            src_ref=x_ref,
            dst_ref=held.at[slot],
            send_sem=send_sem.at[at],
            recv_sem=recv_sem.at[at],
            device_id={axis: peer},
            device_id_type=MESH,
        )
        copy.start()
        copies.append(copy)
    held[slot] = x_ref[...]
    for copy in copies:
        copy.wait()
    if combine == 'sum':
        total = held[0]
        for src in range(1, size):
            total = total + held[src]
        out_ref[...] = total
    else:
        top = held[0]
        for src in range(1, size):
            top = jnp.maximum(top, held[src])
        total = jnp.exp2(held[0] - top)
        for src in range(1, size):
            total = total + jnp.exp2(held[src] - top)
        out_ref[...] = top + jnp.log2(total)


def exchange(vals, axis, size, stride, combine, collective_id):
    return pl.pallas_call(
        functools.partial(exchange_kernel, axis, size, stride, combine),
        out_shape=jax.ShapeDtypeStruct(vals.shape, vals.dtype),
        in_specs=[pl.BlockSpec(memory_space=pltpu.VMEM)],
        out_specs=pl.BlockSpec(memory_space=pltpu.VMEM),
        scratch_shapes=[
            pltpu.VMEM((size,) + vals.shape, vals.dtype),
            pltpu.SemaphoreType.DMA((size - 1,)),
            pltpu.SemaphoreType.DMA((size - 1,)),
        ],
        compiler_params=pltpu.CompilerParams(collective_id=collective_id, has_side_effects=True),
        cost_estimate=pl.CostEstimate(flops=8_000_000, bytes_accessed=2 * vals.size * 4, transcendentals=0),
    )(vals)


def rope_kernel(head_dim, q_ref, k_ref, q_inv, k_inv, q_gain, k_gain, cos_ref, sin_ref, q_out, k_out):
    cos_tab, sin_tab = cos_ref[...], sin_ref[...]
    for raw, inv, gain, out in ((q_ref, q_inv, q_gain, q_out), (k_ref, k_inv, k_gain, k_out)):
        scale = inv[...]
        for head in range(raw.shape[1] // head_dim):
            cols = slice(head * head_dim, (head + 1) * head_dim)
            vals = raw[:, cols] * scale * gain[:, cols]
            out[:, cols] = (vals * cos_tab + pltpu.roll(vals, head_dim // 2, 1) * sin_tab).astype(out.dtype)


def norm_rope(q_raw, k_raw, q_inv, k_inv, q_gain, k_gain, cos_tab, sin_tab, head_dim):
    tokens, q_width = q_raw.shape
    k_width = k_raw.shape[1]
    tile = math.gcd(tokens, TOKEN_TILE)
    by_token = lambda width: pl.BlockSpec((tile, width), lambda i: (i, 0))
    whole = lambda width: pl.BlockSpec((1, width), lambda i: (0, 0))
    return pl.pallas_call(
        functools.partial(rope_kernel, head_dim),
        grid=(tokens // tile,),
        out_shape=(jax.ShapeDtypeStruct(q_raw.shape, jnp.bfloat16), jax.ShapeDtypeStruct(k_raw.shape, jnp.bfloat16)),
        in_specs=[by_token(q_width), by_token(k_width), by_token(head_dim), by_token(head_dim), whole(q_width), whole(k_width), by_token(head_dim), by_token(head_dim)],
        out_specs=(by_token(q_width), by_token(k_width)),
        compiler_params=pltpu.CompilerParams(vmem_limit_bytes=VMEM_BYTES),
        cost_estimate=pl.CostEstimate(flops=tokens * q_width * 8, bytes_accessed=tokens * (q_width + k_width) * 6, transcendentals=0),
        name='norm_rope',
    )(q_raw, k_raw, q_inv, k_inv, q_gain, k_gain, cos_tab, sin_tab)


def attention_kernel(row0, groups, exp_scale, info, q_ref, k_ref, v_ref, kc_ref, vc_ref, own_ref, other_ref, stats_ref, vt_ref, s_even, s_odd):
    blocks, _, chunk_dev, _ = q_ref.shape
    cache_dev, head_dim = k_ref.shape[2], k_ref.shape[3]
    core = lax.rem(info[0], CORES)
    key_base = info[0] * chunk_dev
    valid = info[1 + row0 + pl.program_id(0)]
    tiles = groups * CORES
    q_size = blocks // CORES * chunk_dev
    piece = math.gcd(cache_dev, KEY_PIECE)
    scratch = (s_even, s_odd)

    def q_tile(tile):
        side, group = divmod(tile, groups)
        first = lax.rem(core + side, CORES)
        cols = slice(group * head_dim, (group + 1) * head_dim)
        return jnp.concatenate([q_ref[first + step, 0, :, cols] for step in range(0, blocks, CORES)], axis=0)

    def scores(keys, q_vals):
        return lax.dot_general(keys, q_vals, (((1,), (1,)), ((), ())), preferred_element_type=jnp.float32)

    def fold(vals):
        return jnp.max(vals.reshape(vals.shape[0] // 8, 8, q_size), axis=0)

    def chunk_scores(tile, q_vals):
        vals = scores(kc_ref[0], q_vals)
        key_index = key_base + lax.broadcasted_iota(jnp.int32, vals.shape, 0)
        lane = lax.broadcasted_iota(jnp.int32, vals.shape, 1)
        block = (lane // chunk_dev) * CORES + lax.rem(core + tile // groups, CORES)
        query_index = block * chunk_dev + lane % chunk_dev
        vals = jnp.where(key_index <= query_index, vals, MASK_VALUE)
        scratch[tile % 2][cache_dev:cache_dev + chunk_dev, :] = vals
        return fold(vals)

    def cache_scores(tile, q_vals, first, masked):
        vals = scores(k_ref[0, 0, first:first + piece, :], q_vals)
        if masked:
            slot = first + lax.broadcasted_iota(jnp.int32, vals.shape, 0)
            vals = jnp.where(slot < valid, vals, MASK_VALUE)
        scratch[tile % 2][first:first + piece, :] = vals
        return fold(vals)

    def weights(tile, first, size, top_scaled):
        probs = jnp.exp2(scratch[tile % 2][first:first + size, :] * exp_scale - top_scaled)
        return probs.astype(jnp.bfloat16), jnp.sum(probs.reshape(size // 8, 8, q_size), axis=0)

    def run(masked, with_cache):
        firsts = range(0, cache_dev, piece) if with_cache else ()

        def first_scores(tile):
            q_vals = q_tile(tile)
            top = chunk_scores(tile, q_vals)
            for first in firsts:
                top = jnp.maximum(top, cache_scores(tile, q_vals, first, masked))
            return top

        top = first_scores(0)
        for tile in range(tiles):
            top_scaled = jnp.max(top, axis=0, keepdims=True) * exp_scale
            more = tile + 1 < tiles
            if more:
                q_next = q_tile(tile + 1)
                top = chunk_scores(tile + 1, q_next)
            probs, den = weights(tile, cache_dev, chunk_dev, top_scaled)
            num = lax.dot_general(vc_ref[0], probs, (((0,), (0,)), ((), ())), preferred_element_type=jnp.float32)
            for first in firsts:
                if more:
                    top = jnp.maximum(top, cache_scores(tile + 1, q_next, first, masked))
                probs, part = weights(tile, first, piece, top_scaled)
                den = den + part
                num = num + jnp.dot(vt_ref[:, first:first + piece], probs, preferred_element_type=jnp.float32)
            (own_ref, other_ref)[tile // groups][0, 0, tile % groups] = num
            stats_ref[0, 0, tile:tile + 1, :] = top_scaled
            stats_ref[0, 0, tiles + tile:tiles + tile + 1, :] = top_scaled + jnp.log2(jnp.sum(den, axis=0, keepdims=True))

    @pl.when(valid > 0)
    def _():
        vt_ref[...] = v_ref[0, 0].T

    pl.when(valid >= cache_dev)(lambda: run(False, True))
    pl.when(jnp.logical_and(valid > 0, valid < cache_dev))(lambda: run(True, True))
    pl.when(valid <= 0)(lambda: run(False, False))


def attention(info, q_all, k_heads, v_heads, chunk_k, chunk_v, row0, groups):
    blocks, rows, chunk_dev, q_width = q_all.shape
    _, kv_local, cache_dev, head_dim = k_heads.shape
    q_size = blocks // CORES * chunk_dev
    q_head_width = q_width // kv_local
    num = jax.ShapeDtypeStruct((rows, kv_local, groups, head_dim, q_size), jnp.float32)
    num_spec = pl.BlockSpec((1, 1, groups, head_dim, q_size), lambda r, h, _: (r, h, 0, 0, 0))
    stats_rows = 2 * CORES * groups
    cache_spec = pl.BlockSpec((1, 1, cache_dev, head_dim), lambda r, h, _: (row0 + r, h, 0, 0))
    chunk_spec = pl.BlockSpec((1, chunk_dev, head_dim), lambda r, h, _: (row0 + r, 0, h))
    scores = rows * q_width // head_dim * blocks * chunk_dev * (cache_dev + chunk_dev)
    return pl.pallas_call(
        functools.partial(attention_kernel, row0, groups, math.log2(math.e) * head_dim ** -0.5),
        out_shape=(num, num, jax.ShapeDtypeStruct((rows, kv_local, stats_rows, q_size), jnp.float32)),
        grid_spec=pltpu.PrefetchScalarGridSpec(
            num_scalar_prefetch=1,
            grid=(rows, kv_local),
            in_specs=[
                pl.BlockSpec((blocks, 1, chunk_dev, q_head_width), lambda r, h, _: (0, r, 0, h)),
                cache_spec, cache_spec, chunk_spec, chunk_spec,
            ],
            out_specs=(num_spec, num_spec, pl.BlockSpec((1, 1, stats_rows, q_size), lambda r, h, _: (r, h, 0, 0))),
            scratch_shapes=[
                pltpu.VMEM((head_dim, cache_dev), jnp.bfloat16),
                pltpu.VMEM((cache_dev + chunk_dev, q_size), jnp.float32),
                pltpu.VMEM((cache_dev + chunk_dev, q_size), jnp.float32),
            ],
        ),
        compiler_params=pltpu.CompilerParams(vmem_limit_bytes=VMEM_BYTES),
        cost_estimate=pl.CostEstimate(flops=1_000_000, bytes_accessed=scores // 8, transcendentals=0),
        name='attention',
    )(info, q_all, k_heads, v_heads, chunk_k, chunk_v)


def merge_kernel(own_ref, peer_ref, own_stats, peer_stats, lse_ref, out_ref):
    _, kv_local, groups, head_dim, _ = own_ref.shape
    blocks, chunk_dev, _ = out_ref.shape
    for kv_head in range(kv_local):
        lse = lse_ref[0, kv_head]
        own_factor = jnp.exp2(own_stats[0, kv_head, :groups] - lse)
        peer_factor = jnp.exp2(peer_stats[0, kv_head, groups:2 * groups] - lse)
        for group in range(groups):
            head = kv_head * groups + group
            at = slice(group, group + 1)
            both = own_ref[0, kv_head, group] * own_factor[at] + peer_ref[0, kv_head, group] * peer_factor[at]
            out_ref[:, :, head * head_dim:(head + 1) * head_dim] = both.T.reshape(blocks, chunk_dev, head_dim)


def merge_parts(own, peer, own_stats, peer_stats, lse, chunk_dev):
    rows, kv_local, groups, head_dim, q_size = own.shape
    blocks = q_size // chunk_dev
    width = kv_local * groups * head_dim
    by_row = lambda shape: pl.BlockSpec((1,) + shape[1:], lambda r: (r,) + (0,) * (len(shape) - 1))
    return pl.pallas_call(
        merge_kernel,
        grid=(rows,),
        out_shape=jax.ShapeDtypeStruct((blocks, rows * chunk_dev, width), jnp.float32),
        in_specs=[by_row(own.shape), by_row(own.shape), by_row(own_stats.shape), by_row(own_stats.shape), by_row(lse.shape)],
        out_specs=pl.BlockSpec((blocks, chunk_dev, width), lambda r: (0, r, 0)),
        compiler_params=pltpu.CompilerParams(vmem_limit_bytes=VMEM_BYTES),
        cost_estimate=pl.CostEstimate(flops=own.size * 8, bytes_accessed=own.size * 12, transcendentals=0),
        name='merge_parts',
    )(own, peer, own_stats, peer_stats, lse)


def out_kernel(tp_size, *refs):
    info = refs[0]
    w_refs, o_refs = refs[1:1 + 2 * tp_size - 1], refs[2 * tp_size:2 * tp_size + tp_size + 1]
    x_ref, gain_ref = refs[3 * tp_size + 1:3 * tp_size + 3]
    out_ref, w_held, o_held, w_sem, o_sem = refs[-5:]
    me, core = info[0], info[1]
    w_half = w_held.shape[1] // CORES
    o_half = o_held.shape[1] // 2
    tile = x_ref.shape[0]
    step = pl.program_id(0)

    @pl.when(step == 0)
    def _():
        for away in range(tp_size):
            slot = lax.rem(me + away, tp_size)
            if away == tp_size // 2:
                for part in range(2):
                    pltpu.make_async_copy(o_refs[away + part], o_held.at[slot, pl.ds(part * o_half, o_half)], o_sem.at[slot]).start()
            else:
                pltpu.make_async_copy(o_refs[away + (away > tp_size // 2)], o_held.at[slot], o_sem.at[slot]).start()
        for away in range(tp_size):
            slot = lax.rem(me + away, tp_size)
            if away == 0:
                pltpu.make_async_copy(w_refs[0], w_held.at[slot], w_sem.at[slot]).start()
            else:
                for part in range(CORES):
                    first = pl.multiple_of(lax.rem(core + part, CORES) * w_half, 8)
                    pltpu.make_async_copy(w_refs[CORES * away - 1 + part], w_held.at[slot, pl.ds(first, w_half)], w_sem.at[slot]).start()

    total = None
    for src in range(tp_size):
        @pl.when(step == 0)
        def _():
            pltpu.make_async_copy(o_held.at[src], o_held.at[src], o_sem.at[src]).wait()
            pltpu.make_async_copy(w_held.at[src], w_held.at[src], w_sem.at[src]).wait()

        part = jnp.dot(o_held[src, pl.ds(pl.multiple_of(step * tile, tile), tile), :], w_held[src], preferred_element_type=jnp.float32)
        total = part if total is None else total + part
    normed = total * lax.rsqrt(jnp.mean(total * total, axis=-1, keepdims=True) + NORM_EPS) * gain_ref[...]
    out_ref[...] = (x_ref[...].astype(jnp.float32) + normed).astype(out_ref.dtype)


def project_out(info, w_parts, o_parts, x_tokens, gain, earlier, token0):
    tp_size = (len(w_parts) + 1) // CORES
    tokens, width = o_parts[0].shape
    model_dim = x_tokens.shape[1]
    tile = math.gcd(tokens, TOKEN_TILE)
    shift = token0 // tile
    here = lambda i, _: (shift + i, 0)
    in_hbm = pl.BlockSpec(memory_space=pl.ANY)
    in_specs = [in_hbm] * (len(w_parts) + len(o_parts)) + [pl.BlockSpec((tile, model_dim), here), pl.BlockSpec((1, model_dim), lambda i, _: (0, 0))]
    operands = [info, *w_parts, *o_parts, x_tokens, gain]
    aliases = {}
    if earlier is not None:
        in_specs.append(in_hbm)
        aliases = {len(operands): 0}
        operands.append(earlier)
    return pl.pallas_call(
        functools.partial(out_kernel, tp_size),
        out_shape=jax.ShapeDtypeStruct(x_tokens.shape, jnp.bfloat16),
        grid_spec=pltpu.PrefetchScalarGridSpec(
            num_scalar_prefetch=1,
            grid=(tokens // tile,),
            in_specs=in_specs,
            out_specs=pl.BlockSpec((tile, model_dim), here),
            scratch_shapes=[
                pltpu.VMEM((tp_size, width, model_dim), jnp.bfloat16),
                pltpu.VMEM((tp_size, tokens, width), jnp.bfloat16),
                pltpu.SemaphoreType.DMA((tp_size,)),
                pltpu.SemaphoreType.DMA((tp_size,)),
            ],
        ),
        input_output_aliases=aliases,
        compiler_params=pltpu.CompilerParams(vmem_limit_bytes=VMEM_BYTES),
        cost_estimate=pl.CostEstimate(flops=2 * tokens * tp_size * width * model_dim, bytes_accessed=8 * width * model_dim, transcendentals=0),
        name='project_out',
    )(*operands)


def ring(size, shift):
    return [(i, (i + shift) % size) for i in range(size)]


def gather_by_distance(vals, axis, size):
    mid = vals.shape[0] // 2
    below = lax.ppermute(vals, axis, ring(size, 1))
    above = lax.ppermute(vals, axis, ring(size, -1))
    far_low = lax.ppermute(below[:mid], axis, ring(size, 1))
    far_high = lax.ppermute(above[mid:], axis, ring(size, -1))
    return [vals, above, far_low, far_high, below]


def solution(mesh):
    cp_size = mesh.shape['cp']
    tp_size = mesh.shape['tp']

    def sublayer(x_chunk, w_query, w_key, w_value, w_out, q_gain, k_gain, post_gain, cache_k, cache_v, prefix_len):
        batch_rows, chunk_dev, model_dim = x_chunk.shape
        cache_dev, kv_local, head_dim = cache_k.shape[1:]
        q_width, k_width = w_query.shape[1], w_key.shape[1]
        groups = q_width // k_width
        cp_index = lax.axis_index('cp')
        tp_index = lax.axis_index('tp')
        rows = batch_rows // ROW_CHUNKS
        tokens = x_chunk.reshape(batch_rows * chunk_dev, model_dim)

        core_index = cp_index % CORES
        w_piece = w_out.shape[0] // CORES
        partner = [(i, i + 1 - 2 * (i % CORES)) for i in range(cp_size)]
        same_core = [list(range(core, cp_size, CORES)) for core in range(CORES)]

        q_raw = jnp.dot(tokens, w_query, preferred_element_type=jnp.float32)
        q_squares = jnp.sum(q_raw * q_raw, axis=-1)
        k_raw = jnp.dot(tokens, w_key, preferred_element_type=jnp.float32)
        chunk_v = jnp.dot(tokens, w_value, preferred_element_type=jnp.float32).astype(jnp.bfloat16)
        squares = jnp.stack([q_squares, jnp.sum(k_raw * k_raw, axis=-1)])
        square_sums = exchange(squares.reshape(-1, 128), 'tp', tp_size, 1, 'sum', 0).reshape(squares.shape)
        w_own = lax.dynamic_slice_in_dim(w_out, core_index * w_piece, w_piece, axis=0)
        w_own, square_sums = lax.optimization_barrier((w_own, square_sums))
        w_mine = [lax.ppermute(w_own, 'tp', ring(tp_size, -away)) for away in range(1, tp_size)]
        q_inv = lax.rsqrt(square_sums[0] / (q_width * tp_size) + NORM_EPS)
        k_inv = lax.rsqrt(square_sums[1] / (k_width * tp_size) + NORM_EPS)
        wide = lambda vec: jnp.broadcast_to(vec[:, None], (vec.shape[0], head_dim))
        positions = (prefix_len[:, None] + cp_index * chunk_dev + jnp.arange(chunk_dev, dtype=jnp.int32)[None, :]).reshape(-1)
        cos_tab, sin_tab = rope_tables(positions, head_dim)
        q_new, chunk_k = norm_rope(
            q_raw, k_raw, wide(q_inv), wide(k_inv), q_gain.astype(jnp.float32)[None, :], k_gain.astype(jnp.float32)[None, :], cos_tab, sin_tab, head_dim
        )
        q_new = q_new.reshape(batch_rows, chunk_dev, q_width)
        k_rows = chunk_k.reshape(batch_rows, chunk_dev, k_width)
        v_rows = chunk_v.reshape(batch_rows, chunk_dev, k_width)
        k_heads = jnp.transpose(cache_k, (0, 2, 1, 3))
        v_heads = jnp.transpose(cache_v, (0, 2, 1, 3))
        valid = jnp.clip(prefix_len - cp_index * cache_dev, 0, cache_dev)
        info = jnp.concatenate([jnp.reshape(cp_index, (1,)), valid]).astype(jnp.int32)
        tp_info = jnp.stack([tp_index, core_index]).astype(jnp.int32)
        post = post_gain.astype(jnp.float32)[None, :]

        gathered = [lax.all_gather(q_new[c * rows:(c + 1) * rows], 'cp', axis=0, tiled=False) for c in range(ROW_CHUNKS)]
        gathered[1:] = lax.optimization_barrier(gathered[1:])
        parts = []
        for c in range(ROW_CHUNKS):
            own, other, stats = attention(info, gathered[c], k_heads, v_heads, k_rows, v_rows, c * rows, groups)
            if c == SWAP_AT:
                w_mine, other = lax.optimization_barrier((w_mine, other))
                w_theirs = [lax.ppermute(piece, 'cp', partner) for piece in w_mine]
                w_parts = [w_out] + [piece for pair in zip(w_mine, w_theirs) for piece in pair]
            peer = lax.ppermute(other, 'cp', partner)
            peer_stats = lax.ppermute(stats, 'cp', partner)
            own_lse, peer_lse = stats[:, :, 2 * groups:3 * groups], peer_stats[:, :, 3 * groups:]
            top = jnp.maximum(own_lse, peer_lse)
            pair_lse = top + jnp.log2(jnp.exp2(own_lse - top) + jnp.exp2(peer_lse - top))
            lse = exchange(pair_lse.reshape(-1, pair_lse.shape[-1]), 'cp', cp_size // CORES, CORES, 'lse', 1 + c).reshape(pair_lse.shape)
            merged = merge_parts(own, peer, stats, peer_stats, lse, chunk_dev)
            parts.append(lax.psum_scatter(merged, 'cp', scatter_dimension=0, axis_index_groups=same_core, tiled=False))
        block_out = None
        for c in range(ROW_CHUNKS):
            part = parts[c]
            if c == ROW_CHUNKS - 1:
                part, block_out = lax.optimization_barrier((part, block_out))
            o_parts = gather_by_distance(part.astype(jnp.bfloat16), 'tp', tp_size)
            block_out = project_out(tp_info, w_parts, o_parts, tokens, post, block_out, c * rows * chunk_dev)
        heads_shape = (batch_rows, chunk_dev, kv_local, head_dim)
        return block_out.reshape(x_chunk.shape), chunk_k.reshape(heads_shape), chunk_v.reshape(heads_shape)

    x_spec = P('dp', 'cp', None)
    head_spec = P('dp', 'cp', 'tp', None)
    in_specs = (x_spec, P(None, 'tp'), P(None, 'tp'), P(None, 'tp'), P('tp', None), P('tp'), P('tp'), P(None), head_spec, head_spec, P('dp'))
    out_specs = (x_spec, head_spec, head_spec)
    return jax.shard_map(sublayer, mesh=mesh, in_specs=in_specs, out_specs=out_specs, check_vma=False)
```
